32 devices in a mesh: dp: 4 (over y, x), group: 8 (over z, core).
Axes of the slice: x: 2, y: 2, z: 4, core: 2. Of those that a mesh axis runs over, the one named last changes fastest.
Arguments:
- tokens: bfloat16 [2048, 5120], P('dp'), may hold values from -6 to 6
- frame_mask: int32 [2048], P('dp'), may hold values 0 or 1
- cotangent: bfloat16 [2048, 5120], P('dp'), may hold values from -0.625 to 0.625
- up_weight: bfloat16 [5120, 8192], P('dp', 'group'), may hold values from -0.078125 to 0.078125
- down_weight: bfloat16 [5120, 8192], P('dp', 'group'), may hold values from -0.0625 to 0.0625
- snap_params: bfloat16 [8, 32768], P(None, ('dp', 'group')), may hold values from -6 to 6
- first_moment: float32 [8, 32768], P(None, ('dp', 'group')), may hold values from -6 to 6
- second_moment: float32 [8, 32768], P(None, ('dp', 'group')), may hold values from 0.01 to 4
- range_of_writer: int32 [8], replicated, may hold values from 0 to 7, each once
Outputs:
- grad_up: float32 [5120, 8192], P('dp', 'group')
- grad_down: float32 [5120, 8192], P('dp', 'group')
- written_params: bfloat16 [8, 32768], P('group', 'dp')
- written_moments: float32 [2, 8, 32768], P(None, 'group', 'dp')
The draws below stay inside these ranges and needn't reach their ends.
Inputs may be any that keep to these rules, and one draw needn't show every extreme that they name: `range_of_writer`: each of the 8 ranges is named by exactly one owner.
All inputs are finite; a program needn't handle non-finite values. No bound on the sum of `frame_mask` on one device may be relied on, other than what follows from the above.
Results may differ from the reference program's by a relative error of at most 0.017.
Values may be sent and summed in bfloat16 or wider, within the bound.
No kernel may reach another device: no remote copies, remote signals or barrier semaphores. Data moves between devices by JAX's collectives and lax.ppermute only.
A program may use at most 128 MiB of HBM per device.

```python
import math
import jax
import jax.numpy as jnp
from jax import lax

D = 5120
FF = 8192
TOK_DEV = 512
TOKENS = 2048
RANGES = 8
FLAT = 32768
N_DP = 4
N_GROUP = 8


def set_ends(values, own_key, low, top_value):
    spot = [jax.random.randint(jax.random.fold_in(own_key, axis), (), 0, length) for axis, length in enumerate(values.shape)]
    widest = values.shape.index(max(values.shape))
    beside = spot[:widest] + [(spot[widest] + 1) % values.shape[widest]] + spot[widest + 1:]
    return values.at[tuple(spot)].set(low).at[tuple(beside)].set(top_value)


def raised(entries, key, source, target, blocks, factor):
    owner, partner = [(jnp.arange(entries.shape[axis_at]) // (entries.shape[axis_at] // blocks)).reshape([-1 if axis == axis_at else 1 for axis in range(entries.ndim)]) for axis_at in (source, target)]
    chosen = jax.random.permutation(key, blocks)[partner]
    strong = (owner == chosen) | (owner == (partner + blocks // 2) % blocks)
    return jnp.where(strong, factor * entries, entries)


def levels(rng, shape, cuts, smallest, largest):
    loudness = 1.0
    for dim, shards_of in cuts:
        heights = jax.random.uniform(jax.random.fold_in(jax.random.fold_in(rng, 6), dim), (shards_of,), jnp.float32, smallest / len(cuts), largest / len(cuts))
        loudness = loudness * jnp.repeat(jnp.exp(heights), shape[dim] // shards_of).reshape((-1,) + (1,) * (len(shape) - 1 - dim))
    return loudness


def bell_draw(key, dims, deviation, most, cuts=(), held_as=jnp.bfloat16):
    level = levels(key, dims, cuts, -0.22, 0.18) if cuts else 1.0
    drawn = jax.random.normal(key, dims, jnp.float32) * deviation * level
    return jnp.minimum(jnp.maximum(drawn, -most), most).astype(held_as)


def bell_draw_with(own_key, shape, deviation, reach, split, heavy, kind=jnp.bfloat16):
    array = deviation * jax.random.normal(own_key, shape, jnp.float32)
    if split:
        array = array * levels(own_key, shape, split, -0.22, 0.18)
    return jnp.clip(raised(array, jax.random.fold_in(own_key, 3), *heavy), -reach, reach).astype(kind)


def setup_inputs(seed: int = 0) -> dict:
    seeds = jax.random.split(jax.random.key(seed), 10)
    return {
        "tokens": bell_draw(seeds[0], (TOKENS, D), 1.0, 6.0, ((0, 4),)),
        "frame_mask": set_ends((jax.random.randint(seeds[1], (TOKENS,), 0, 4) < 3).astype(jnp.int32), jax.random.fold_in(seeds[1], 1), 0, 1),
        "cotangent": bell_draw_with(seeds[2], (TOKENS, D), 0.03, 0.625, ((0, 4),), (0, 1, 4, 2.0)),
        "up_weight": bell_draw(seeds[3], (D, FF), D ** -0.5, 0.078125, ((0, 4), (1, 8))),
        "down_weight": bell_draw(seeds[4], (D, FF), FF ** -0.5, 0.0625, ((0, 4), (1, 8))),
        "snap_params": bell_draw(seeds[5], (RANGES, FLAT), 0.5, 6.0, ((1, 32),)),
        "first_moment": bell_draw(seeds[6], (RANGES, FLAT), 0.5, 6.0, ((1, 32),), jnp.float32),
        "second_moment": jnp.clip(jnp.exp(math.log(4.0) - 5.9914646 * jax.random.uniform(seeds[7], (RANGES, FLAT), jnp.float32) ** levels(seeds[7], (RANGES, FLAT), ((1, 32),), -0.2, 0.2)), 0.01, 4.0),
        "range_of_writer": jax.random.permutation(seeds[8], N_GROUP).astype(jnp.int32),
    }


EPS = 1e-06

def normalize(tokens):
    values = tokens.astype(jnp.float32)
    centred = values - lax.optimization_barrier(jnp.mean(values, axis=1, keepdims=True))
    spread = lax.optimization_barrier(jnp.mean(centred * centred, axis=1, keepdims=True))
    return (centred * lax.rsqrt(spread + EPS)).astype(jnp.bfloat16)

def gelu_pair(pre, d_act):
    act, pullback = jax.vjp(lambda v: jax.nn.gelu(v, approximate=True), pre)
    return (act.astype(jnp.bfloat16), pullback(d_act)[0].astype(jnp.bfloat16))

def outer_sum(left, right):
    return lax.dot_general(left, right, (((0,), (0,)), ((), ())), preferred_element_type=jnp.float32)

def reference(tokens, frame_mask, cotangent, up_weight, down_weight, snap_params, first_moment, second_moment, range_of_writer):
    normed = normalize(tokens)
    masked = cotangent * frame_mask[:, None].astype(jnp.bfloat16)
    pre = jnp.dot(normed, up_weight, preferred_element_type=jnp.float32)
    d_act = jnp.dot(masked, down_weight, preferred_element_type=jnp.float32)
    act, grad_pre = gelu_pair(pre, d_act)
    blocks = (normed.reshape(N_DP, TOK_DEV, D), grad_pre.reshape(N_DP, TOK_DEV, FF), masked.reshape(N_DP, TOK_DEV, D), act.reshape(N_DP, TOK_DEV, FF))

    def accumulate(totals, block):
        n_blk, g_blk, m_blk, a_blk = block
        up_part = lax.optimization_barrier(outer_sum(n_blk, g_blk).astype(jnp.bfloat16)).astype(jnp.float32)
        down_part = lax.optimization_barrier(outer_sum(m_blk, a_blk).astype(jnp.bfloat16)).astype(jnp.float32)
        return ((totals[0] + up_part, totals[1] + down_part), None)
    empty = jnp.zeros((D, FF), jnp.float32)
    (grad_up, grad_down), _ = lax.scan(accumulate, (empty, empty), blocks)
    order = range_of_writer.astype(jnp.int32)
    written_params = snap_params[order]
    written_moments = jnp.stack([first_moment[order], second_moment[order]])
    return (grad_up, grad_down, written_params, written_moments)
```

```python
import jax
import jax.numpy as jnp
from jax import lax
from jax.sharding import PartitionSpec as P

EPS = 1e-06


def normalize(tokens):
    values = tokens.astype(jnp.float32)
    centred = values - jnp.mean(values, axis=1, keepdims=True)
    spread = jnp.mean(centred * centred, axis=1, keepdims=True)
    return (centred * lax.rsqrt(spread + EPS)).astype(jnp.bfloat16)


def gelu_pair(pre, d_act):
    act, pullback = jax.vjp(lambda v: jax.nn.gelu(v, approximate=True), pre)
    return (act.astype(jnp.bfloat16), pullback(d_act)[0].astype(jnp.bfloat16))


def outer_sum(left, right):
    return lax.dot_general(
        left, right, (((0,), (0,)), ((), ())), preferred_element_type=jnp.float32
    )


def regroup(snap_params, first_moment, second_moment, range_of_writer):
    parts = [
        jnp.take(part.astype(jnp.bfloat16), range_of_writer, axis=0)
        for part in (snap_params, first_moment, second_moment)
    ]
    got = lax.all_to_all(
        jnp.stack(parts, axis=1), "group", split_axis=0, concat_axis=0, tiled=True
    )
    params, first, second = (got[:, i].reshape(1, -1) for i in range(3))
    moments = jnp.stack([first, second]).astype(first_moment.dtype)
    return (params.astype(snap_params.dtype), moments)


def snake(n):
    if n % 2:
        return list(range(n))
    return list(range(n // 2)) + list(range(n - 1, n // 2 - 1, -1))


def make_per_device(n_dp, n_group):
    ring = snake(n_dp)
    cores = 2 if n_group % 2 == 0 else 1

    def shift(value, by):
        pairs = [(ring[i], ring[(i + by) % n_dp]) for i in range(n_dp)]
        return lax.ppermute(value, "dp", pairs)

    def swap(value):
        return lax.ppermute(value, "group", [(i, i ^ 1) for i in range(n_group)])

    def per_device(
        tokens,
        frame_mask,
        cotangent,
        up_weight,
        down_weight,
        snap_params,
        first_moment,
        second_moment,
        range_of_writer,
    ):
        written = regroup(snap_params, first_moment, second_moment, range_of_writer)
        rows = tokens.shape[0] // cores
        cols = up_weight.shape[0]
        core = lax.axis_index("group") % cores
        where = jnp.argsort(jnp.array(ring))[lax.axis_index("dp")]
        ring_at = jnp.array(ring)

        def block_at(offset):
            return ring_at[(where + offset) % n_dp]

        def half(array, h):
            return lax.dynamic_slice_in_dim(array, ((core + h) % cores) * rows, rows, 0)

        def columns(array, offset):
            return lax.dynamic_slice_in_dim(array, block_at(offset) * cols, cols, 1)

        normed = [normalize(half(tokens, h)) for h in range(cores)]
        masked = [
            half(cotangent, h) * half(frame_mask, h)[:, None].astype(jnp.bfloat16)
            for h in range(cores)
        ]

        def exchange(values, way):
            got = [[columns(v, 0) for v in values]]
            for s in range(1, n_dp):
                direct = shift(columns(values[0], way * s), way * s)
                got.append([direct, swap(direct)] if cores == 2 else [direct])
            return got

        normed_of = exchange(normed, 1)
        masked_of = exchange(masked, -1)

        def reduce_round(blocks, weight, way):
            out = []
            for h in range(cores):
                carry = None
                for s in range(1, n_dp + 1):
                    part = jnp.dot(
                        blocks[s % n_dp][h], weight, preferred_element_type=jnp.float32
                    )
                    if carry is not None:
                        part = part + shift(carry, way).astype(jnp.float32)
                    carry = part.astype(jnp.bfloat16)
                out.append(part)
            return out

        pre = reduce_round(normed_of, up_weight, 1)
        d_act = reduce_round(masked_of, down_weight, -1)
        pairs = [gelu_pair(p, d) for p, d in zip(pre, d_act)]
        act = [a for a, _ in pairs]
        grad_pre = [g for _, g in pairs]

        def gather_round(blocks, mine, way):
            total = None
            for s in range(n_dp):
                part = outer_sum(
                    jnp.concatenate(blocks[s], axis=0),
                    jnp.concatenate(mine, axis=0),
                )
                total = part if total is None else total + part
                if s + 1 < n_dp:
                    mine = [shift(v, way) for v in mine]
            return total

        grad_down = gather_round(masked_of, act, -1)
        grad_up = gather_round(normed_of, grad_pre, 1)
        return (grad_up, grad_down, written[0], written[1])

    return per_device


def solution(mesh):
    placed = (
        P("dp", None),
        P("dp"),
        P("dp", None),
        P("dp", "group"),
        P("dp", "group"),
        P(None, ("dp", "group")),
        P(None, ("dp", "group")),
        P(None, ("dp", "group")),
        P(),
    )
    return jax.shard_map(
        make_per_device(mesh.shape["dp"], mesh.shape["group"]),
        mesh=mesh,
        in_specs=placed,
        out_specs=(P("dp", "group"), P("dp", "group"), P("group", "dp"), P(None, "group", "dp")),
        check_vma=False,
    )
```

```python
import jax
import jax.numpy as jnp
from jax import lax
from jax.sharding import PartitionSpec as P

EPS = 1e-06


def normalize(tokens):
    values = tokens.astype(jnp.float32)
    centred = values - jnp.mean(values, axis=1, keepdims=True)
    spread = jnp.mean(centred * centred, axis=1, keepdims=True)
    return (centred * lax.rsqrt(spread + EPS)).astype(jnp.bfloat16)


def gelu_pair(pre, d_act):
    act, pullback = jax.vjp(lambda v: jax.nn.gelu(v, approximate=True), pre)
    return (act.astype(jnp.bfloat16), pullback(d_act)[0].astype(jnp.bfloat16))


def outer_sum(left, right):
    return lax.dot_general(
        left, right, (((0,), (0,)), ((), ())), preferred_element_type=jnp.float32
    )


def regroup(snap_params, first_moment, second_moment, range_of_writer):
    parts = [
        jnp.take(part.astype(jnp.bfloat16), range_of_writer, axis=0)
        for part in (snap_params, first_moment, second_moment)
    ]
    got = lax.all_to_all(
        jnp.stack(parts, axis=1), "group", split_axis=0, concat_axis=0, tiled=True
    )
    params, first, second = (got[:, i].reshape(1, -1) for i in range(3))
    moments = jnp.stack([first, second]).astype(first_moment.dtype)
    return (params.astype(snap_params.dtype), moments)


def snake(i, n):
    return i if n % 2 else jnp.where(i < n // 2, i, n // 2 + n - 1 - i)


def make_per_device(n_dp, n_group):
    ring = [i if n_dp % 2 or i < n_dp // 2 else n_dp // 2 + n_dp - 1 - i for i in range(n_dp)]
    shares = 4 if n_group % 4 == 0 else 2 if n_group % 2 == 0 else 1
    flips = {4: (0, 2, 1, 3), 2: (0, 1), 1: (0,)}[shares]
    chunks = min(shares, 2)

    def shift(value, by):
        pairs = [(ring[i], ring[(i + by) % n_dp]) for i in range(n_dp)]
        return lax.ppermute(value, "dp", pairs)

    def swap(value, bit):
        return lax.ppermute(value, "group", [(i, i ^ bit) for i in range(n_group)])

    def per_device(
        tokens,
        frame_mask,
        cotangent,
        up_weight,
        down_weight,
        snap_params,
        first_moment,
        second_moment,
        range_of_writer,
    ):
        rows = tokens.shape[0] // shares
        cols = up_weight.shape[0]
        share = lax.axis_index("group") % shares
        where = snake(lax.axis_index("dp"), n_dp)

        def part_of(array, flip):
            return lax.dynamic_slice_in_dim(array, (share ^ flip) * rows, rows, 0)

        def columns(array, offset):
            block = snake((where + offset) % n_dp, n_dp)
            return lax.dynamic_slice_in_dim(array, block * cols, cols, 1)

        def mask(values, flags):
            return values * flags[:, None].astype(jnp.bfloat16)

        def exchange(values, way):
            got = []
            for s in range(1, n_dp):
                first = shift(columns(values, way * s), way * s)
                if shares == 4:
                    first = jnp.concatenate([first, swap(first, 2)], axis=0)
                got.append([first, swap(first, 1)] if shares > 1 else [first])
            return got

        def in_order(values):
            parts = [part_of(values, flip) for flip in flips]
            per = shares // chunks
            return [jnp.concatenate(parts[i * per : (i + 1) * per], axis=0) for i in range(chunks)]

        masked_part = mask(part_of(cotangent, 0), part_of(frame_mask, 0))
        normed_part = normalize(part_of(tokens, 0))
        masked_got = exchange(masked_part, -1)
        normed_got = exchange(normed_part, 1)
        tokens, _ = lax.optimization_barrier((tokens, normed_part))
        masked_of = [in_order(mask(columns(cotangent, 0), frame_mask))] + masked_got
        normed_of = [in_order(columns(normalize(tokens), 0))] + normed_got

        def reduce_round(blocks, weight, way, hook=None):
            out = []
            for h in range(chunks):
                carry = None
                for s in range(1, n_dp + 1):
                    part = jnp.dot(
                        blocks[s % n_dp][h], weight, preferred_element_type=jnp.float32
                    )
                    if carry is not None:
                        part = part + shift(carry, way).astype(jnp.float32)
                    carry = part.astype(jnp.bfloat16)
                    if s == 1 and h == 0 and hook is not None:
                        carry = hook(carry)
                out.append(part)
            return out

        snap = [snap_params, first_moment, second_moment, range_of_writer]

        def after(carry):
            carry, *snap[:] = lax.optimization_barrier((carry, *snap))
            return carry

        pre = reduce_round(normed_of, up_weight, 1, after)
        d_act = reduce_round(masked_of, down_weight, -1)
        written = regroup(*snap)
        pairs = [gelu_pair(p, d) for p, d in zip(pre, d_act)]
        act = [a for a, _ in pairs]
        grad_pre = [g for _, g in pairs]

        def gather_round(blocks, mine, way):
            total = None
            for s in range(n_dp):
                part = outer_sum(
                    jnp.concatenate(blocks[s], axis=0), jnp.concatenate(mine, axis=0)
                )
                total = part if total is None else total + part
                if s + 1 < n_dp:
                    total = lax.optimization_barrier(total)
                    mine = [shift(v, way) for v in mine]
            return total

        grad_down = gather_round(masked_of, act, -1)
        grad_up = gather_round(normed_of, grad_pre, 1)
        return (grad_up, grad_down, written[0], written[1])

    return per_device


def solution(mesh):
    placed = (
        P("dp", None),
        P("dp"),
        P("dp", None),
        P("dp", "group"),
        P("dp", "group"),
        P(None, ("dp", "group")),
        P(None, ("dp", "group")),
        P(None, ("dp", "group")),
        P(),
    )
    return jax.shard_map(
        make_per_device(mesh.shape["dp"], mesh.shape["group"]),
        mesh=mesh,
        in_specs=placed,
        out_specs=(P("dp", "group"), P("dp", "group"), P("group", "dp"), P(None, "group", "dp")),
        check_vma=False,
    )
```
